32 devices in a mesh: seq: 8 (over y, x, core), mp: 4 (over z).
Axes of the slice: x: 2, y: 2, z: 4, core: 2. Of those that a mesh axis runs over, the one named last changes fastest.
Arguments:
- frames: bfloat16 [192, 250, 256], P('seq'), may hold values from -7.5 to 7.5
- intra_qkv: bfloat16 [256, 3, 256], P(None, None, 'mp'), may hold values from -20 to 20
- intra_out: bfloat16 [256, 256], P('mp'), may hold values from -0.375 to 0.375
- intra_up: bfloat16 [256, 1024], P(None, 'mp'), may hold values from -0.375 to 0.375
- intra_down: bfloat16 [1024, 256], P('mp'), may hold values from -0.1875 to 0.1875
- inter_qkv: bfloat16 [256, 3, 256], P(None, None, 'mp'), may hold values from -20 to 20
- inter_out: bfloat16 [256, 256], P('mp'), may hold values from -0.375 to 0.375
- inter_up: bfloat16 [256, 1024], P(None, 'mp'), may hold values from -0.375 to 0.375
- inter_down: bfloat16 [1024, 256], P('mp'), may hold values from -0.1875 to 0.1875
Outputs:
- margin_sum: bfloat16 [24000, 256], P('seq')
The draws below stay inside these ranges and needn't reach their ends.
All inputs are finite; a program needn't handle non-finite values.
Results may differ from the reference program's by a relative error of at most 0.014.
Values may be sent and summed in bfloat16 or wider, within the bound.
A program may use at most 128 MiB of HBM per device.

```python
import jax
import jax.numpy as jnp
from jax import lax

D = 256
HEADS = 8
HD = 32
FF = 1024
K = 250
STRETCHES = 192


def draw_frames(key, part):
    keyed = jax.random.fold_in(key, 11)
    first = jax.random.fold_in(keyed, 0)
    values = jax.random.normal(first, (STRETCHES, K, D), jnp.float32)
    return jnp.clip(values, -7.5, 7.5).astype(jnp.bfloat16)


def attention_weights(key, salt):
    keyed = jax.random.fold_in(key, salt)
    first = jax.random.fold_in(keyed, 0)
    weights = jax.random.normal(first, (D, 3, D), jnp.float32) * D ** (-0.5)
    return jnp.clip(weights, -20.0, 20.0).astype(jnp.bfloat16)


def draw_intra_qkv(key, part):
    return attention_weights(key, 23)


def draw_inter_qkv(key, part):
    return attention_weights(key, 37)


def level_of(rng, shape, cuts, low, largest):
    gain, own = 1.0, jax.random.fold_in(rng, 6)
    for position, parts in cuts:
        steps = jnp.exp(jax.random.uniform(jax.random.fold_in(own, position), (parts,), jnp.float32, low / len(cuts), largest / len(cuts)))
        gain = gain * jnp.repeat(steps, shape[position] // parts).reshape([-1 if axis == position else 1 for axis in range(len(shape))])
    return gain


def centred(own_key, extent, width, most, cuts=(), dtype=jnp.bfloat16):
    result = jax.random.normal(own_key, extent, jnp.float32) * width
    if len(cuts) > 0:
        result = level_of(own_key, extent, cuts, -0.22, 0.18) * result
    return jnp.clip(result, min=-most, max=most).astype(dtype)


def setup_inputs(seed: int = 0) -> dict:
    streams_of = jax.random.split(jax.random.key(seed), 10)
    return {
        "frames": draw_frames(jax.random.fold_in(streams_of[9], 71), 0),
        "intra_qkv": draw_intra_qkv(jax.random.fold_in(streams_of[9], 71), 0),
        "intra_out": centred(streams_of[2], (D, D), D ** -0.5, 0.375, ((0, 4),)),
        "intra_up": centred(streams_of[3], (D, FF), D ** -0.5, 0.375, ((1, 4),)),
        "intra_down": centred(streams_of[4], (FF, D), FF ** -0.5, 0.1875, ((0, 4),)),
        "inter_qkv": draw_inter_qkv(jax.random.fold_in(streams_of[9], 71), 0),
        "inter_out": centred(streams_of[6], (D, D), D ** -0.5, 0.375, ((0, 4),)),
        "inter_up": centred(streams_of[7], (D, FF), D ** -0.5, 0.375, ((1, 4),)),
        "inter_down": centred(streams_of[8], (FF, D), FF ** -0.5, 0.1875, ((0, 4),)),
    }


def layer_norm(values):
    values = values.astype(jnp.float32)
    centre = values - lax.optimization_barrier(jnp.mean(values, axis=-1, keepdims=True))
    spread = lax.optimization_barrier(jnp.mean(centre * centre, axis=-1, keepdims=True))
    return (centre * lax.rsqrt(spread + 1e-05)).astype(jnp.bfloat16)

def attend(query_rows, key_rows, value_rows):
    factor = HD ** (-0.5)
    scores = jnp.einsum('bqhe,bkhe->bhqk', query_rows.astype(jnp.float32), key_rows.astype(jnp.float32)) * factor
    scores = scores - lax.optimization_barrier(jnp.max(scores, axis=-1, keepdims=True))
    weights = jnp.exp(scores)
    weights = (weights / lax.optimization_barrier(jnp.sum(weights, axis=-1, keepdims=True))).astype(jnp.bfloat16)
    return jnp.einsum('bhqk,bkhe->bqhe', weights.astype(jnp.float32), value_rows.astype(jnp.float32)).astype(jnp.bfloat16)

def transformer(stream, qkv_weight, out_weight, up_weight, down_weight):
    leading, within = (stream.shape[0], stream.shape[1])
    normed = layer_norm(stream)
    projected = jnp.einsum('bld,dtj->tblj', normed.astype(jnp.float32), qkv_weight.astype(jnp.float32)).astype(jnp.bfloat16)
    projected = projected.reshape(3, leading // 2, 2, within, HEADS, HD)
    attended = lax.map(lambda pieces: attend(pieces[0], pieces[1], pieces[2]), (projected[0], projected[1], projected[2]))
    attended = attended.reshape(leading, within, D)
    branch = jnp.einsum('bld,de->ble', attended.astype(jnp.float32), out_weight.astype(jnp.float32))
    middle = (stream.astype(jnp.float32) + branch).astype(jnp.bfloat16)
    normed = layer_norm(middle)
    hidden = jax.nn.relu(jnp.einsum('bld,df->blf', normed.astype(jnp.float32), up_weight.astype(jnp.float32))).astype(jnp.bfloat16)
    branch = jnp.einsum('blf,fd->bld', hidden.astype(jnp.float32), down_weight.astype(jnp.float32))
    return (middle.astype(jnp.float32) + branch).astype(jnp.bfloat16)

def reference(frames, intra_qkv, intra_out, intra_up, intra_down, inter_qkv, inter_out, inter_up, inter_down):
    stream = transformer(frames, intra_qkv, intra_out, intra_up, intra_down)
    across = transformer(jnp.transpose(stream, (1, 0, 2)), inter_qkv, inter_out, inter_up, inter_down)
    stream = jnp.transpose(across, (1, 0, 2))
    hop_len = K // 2
    tail_rows = stream[:, hop_len:]
    earlier = jnp.concatenate([jnp.zeros((1, hop_len, D), jnp.bfloat16), tail_rows[:-1]], axis=0)
    summed = stream[:, :hop_len].astype(jnp.float32) + earlier.astype(jnp.float32)
    return summed.astype(jnp.bfloat16).reshape(STRETCHES * hop_len, D)
```

```python
import functools

import jax
import jax.numpy as jnp
from jax import lax
from jax.experimental import pallas as pl
from jax.experimental.pallas import tpu as pltpu
from jax.sharding import PartitionSpec as P

HEADS = 8
HD = 32
LANES = 128
TILE = 8
MESH = pl.DeviceIdType.MESH


def normed_rows(values):
    centre = values - jnp.mean(values, axis=-1, keepdims=True)
    spread = jnp.mean(centre * centre, axis=-1, keepdims=True)
    return (centre * lax.rsqrt(spread + 1e-05)).astype(jnp.bfloat16)


def dot(a, b):
    return jnp.dot(a, b, preferred_element_type=jnp.float32)


def block_rows(rows, qkv, out, up, down, bias):
    width = rows.shape[-1]
    wide = rows.astype(jnp.float32)
    projected = dot(normed_rows(wide), qkv).astype(jnp.bfloat16)
    lane_head = lax.broadcasted_iota(jnp.int32, (1, LANES), 1) // HD
    groups = []
    for g in range(width // LANES):
        q = projected[:, g * LANES : (g + 1) * LANES]
        k = projected[:, width + g * LANES : width + (g + 1) * LANES]
        v = projected[:, 2 * width + g * LANES : 2 * width + (g + 1) * LANES]
        total = None
        for h in range(LANES // HD):
            own = (lane_head == h).astype(jnp.float32)
            scores = lax.dot_general(
                q * own.astype(jnp.bfloat16),
                k,
                (((1,), (1,)), ((), ())),
                preferred_element_type=jnp.float32,
            )
            if bias is not None:
                scores = scores + bias
            scores = scores - jnp.max(scores, axis=-1, keepdims=True)
            weights = jnp.exp(scores * (HD**-0.5))
            scale = 1.0 / jnp.sum(weights, axis=-1, keepdims=True)
            part = dot(weights.astype(jnp.bfloat16), v) * (scale * own)
            total = part if total is None else total + part
        groups.append(total.astype(jnp.bfloat16))
    attended = jnp.concatenate(groups, axis=-1)
    middle = (wide + dot(attended, out)).astype(jnp.bfloat16)
    wide = middle.astype(jnp.float32)
    hidden = jnp.maximum(dot(normed_rows(wide), up), 0.0).astype(jnp.bfloat16)
    return wide + dot(hidden, down)


def source_of(slots, hop, per):
    r = slots // (2 * per) * per + slots % per
    return jnp.where(r < hop, r + jnp.where(slots % (2 * per) < per, 0, hop), -1)


def intra_kernel(hop, per, x_ref, qkv, out, up, down, o_ref):
    frames = x_ref.shape[1]
    peers = o_ref.shape[0]
    padded = peers * 2 * per
    source = source_of(lax.broadcasted_iota(jnp.int32, (padded, frames), 0), hop, per)
    pick = (source == lax.broadcasted_iota(jnp.int32, (padded, frames), 1)).astype(jnp.bfloat16)
    rows = dot(pick, x_ref[0]).astype(jnp.bfloat16)
    keys = source_of(lax.broadcasted_iota(jnp.int32, (1, padded), 1), hop, per)
    bias = jnp.where(keys >= 0, 0.0, -1e30).astype(jnp.float32)
    result = block_rows(rows, qkv[...], out[...], up[...], down[...], bias)
    o_ref[:, 0] = result.reshape(peers, 2 * per, result.shape[-1]).astype(o_ref.dtype)


def inter_kernel(x_ref, qkv, out, up, down, o_ref):
    ends = []
    for half in range(2):
        result = block_rows(x_ref[half, 0], qkv[...], out[...], up[...], down[...], None)
        ends.append(result.astype(jnp.bfloat16).astype(jnp.float32))
    first, second = ends
    moved = pltpu.roll(second, 1, 0)
    moved = jnp.where(lax.broadcasted_iota(jnp.int32, moved.shape, 0) == 0, 0.0, moved)
    o_ref[0] = (first + moved).astype(o_ref.dtype)


def greet(ids):
    barrier = pltpu.get_barrier_semaphore()
    for peer in ids:
        pl.semaphore_signal(barrier, inc=1, device_id=peer, device_id_type=MESH)
    pl.semaphore_wait(barrier, len(ids))


def exchange_kernel(seq_count, mp_count, src, dst, send, recv, local):
    count = seq_count * mp_count
    me = lax.axis_index("seq") * mp_count + lax.axis_index("mp")
    ranks = [lax.rem(me + k, count) for k in range(1, count)]
    greet([(rank // mp_count, lax.rem(rank, mp_count)) for rank in ranks])
    own = pltpu.make_async_copy(src.at[me], dst.at[me], local)
    own.start()
    copies = []
    for k, rank in enumerate(ranks):
        copies.append(
            pltpu.make_async_remote_copy(
                src_ref=src.at[rank],
                dst_ref=dst.at[me],
                send_sem=send.at[k],
                recv_sem=recv.at[k],
                device_id=(rank // mp_count, lax.rem(rank, mp_count)),
                device_id_type=MESH,
            )
        )
        copies[-1].start()
    own.wait()
    for copy in copies:
        copy.wait()


def return_kernel(seq_count, mp_count, src, dst, send, recv, send_on, recv_on, local):
    seq, mp = lax.axis_index("seq"), lax.axis_index("mp")
    across = [lax.rem(seq + k, seq_count) for k in range(1, seq_count)]
    along = [lax.rem(mp + k, mp_count) for k in range(1, mp_count)]
    greet([(peer, mp) for peer in across] + [(seq, peer) for peer in along])
    own = pltpu.make_async_copy(src.at[:, seq], dst.at[seq, mp], local)
    own.start()
    copies = []
    for k, peer in enumerate(across):
        copies.append(
            pltpu.make_async_remote_copy(
                src_ref=src.at[:, peer],
                dst_ref=dst.at[seq, mp],
                send_sem=send.at[k],
                recv_sem=recv.at[k],
                device_id=(peer, mp),
                device_id_type=MESH,
            )
        )
        copies[-1].start()
    onward = []
    for k in range(seq_count):
        if k == 0:
            own.wait()
        else:
            copies[k - 1].wait_recv()
        slab = dst.at[lax.rem(seq + seq_count - k, seq_count), mp]
        for j, peer in enumerate(along):
            onward.append(
                pltpu.make_async_remote_copy(
                    src_ref=slab,
                    dst_ref=slab,
                    send_sem=send_on.at[k, j],
                    recv_sem=recv_on.at[k, j],
                    device_id=(seq, peer),
                    device_id_type=MESH,
                )
            )
            onward[-1].start()
    for copy in copies:
        copy.wait_send()
    for copy in onward:
        copy.wait()


def gathered(shard, axis):
    peers = lax.axis_size("mp")
    pieces = [shard]
    for by in range(1, peers):
        pieces.append(lax.ppermute(shard, "mp", [(i, (i + by) % peers) for i in range(peers)]))
    return jnp.concatenate(pieces, axis=axis)


def gathered_weights(qkv, out, up, down):
    qkv = gathered(qkv, 2)
    return (
        qkv.reshape(qkv.shape[0], -1),
        gathered(out, 0),
        gathered(up, 1),
        gathered(down, 0),
    )


def whole(array):
    return pl.BlockSpec(array.shape, lambda i: (0,) * array.ndim)


def block_cost(rows, per_group, width, hidden):
    flops = 2 * rows * (width * width * 4 + width * hidden * 2 + 8 * LANES * per_group)
    return pl.CostEstimate(flops=flops, bytes_accessed=rows * width * 4, transcendentals=rows * per_group * 8)


def on_device(
    frames, intra_qkv, intra_out, intra_up, intra_down, inter_qkv, inter_out, inter_up, inter_down
):
    seq_count = lax.axis_size("seq")
    mp_count = lax.axis_size("mp")
    count = seq_count * mp_count
    stretches, length, width = frames.shape
    hop = length // 2
    per = -(-hop // count)
    per = -(-per // (TILE // 2)) * (TILE // 2)
    share = stretches // mp_count
    intra = gathered_weights(intra_qkv, intra_out, intra_up, intra_down)
    inter = gathered_weights(inter_qkv, inter_out, inter_up, inter_down)
    hidden = intra[2].shape[1]
    own = lax.dynamic_slice_in_dim(frames, lax.axis_index("mp") * share, share, 0)
    any_space = pl.BlockSpec(memory_space=pl.ANY)
    parted = pl.pallas_call(
        functools.partial(intra_kernel, hop, per),
        grid=(share,),
        in_specs=[pl.BlockSpec((1, length, width), lambda i: (i, 0, 0))] + [whole(w) for w in intra],
        out_specs=pl.BlockSpec((count, 1, 2 * per, width), lambda i: (0, i, 0, 0)),
        out_shape=jax.ShapeDtypeStruct((count, share, 2 * per, width), jnp.bfloat16),
        cost_estimate=block_cost(share * length, length, width, hidden),
        name="intra",
    )(own, *intra)
    spread = pl.pallas_call(
        functools.partial(exchange_kernel, seq_count, mp_count),
        in_specs=[any_space],
        out_specs=any_space,
        out_shape=jax.ShapeDtypeStruct(parted.shape, jnp.bfloat16),
        scratch_shapes=[
            pltpu.SemaphoreType.DMA((count - 1,)),
            pltpu.SemaphoreType.DMA((count - 1,)),
            pltpu.SemaphoreType.DMA,
        ],
        compiler_params=pltpu.CompilerParams(collective_id=0, has_side_effects=True),
        name="exchange",
    )(parted)
    total = count * share
    spread = jnp.transpose(spread.reshape(total, 2, per, width), (1, 2, 0, 3))
    summed = pl.pallas_call(
        inter_kernel,
        grid=(per,),
        in_specs=[pl.BlockSpec((2, 1, total, width), lambda i: (0, i, 0, 0))]
        + [whole(w) for w in inter],
        out_specs=pl.BlockSpec((1, total, width), lambda i: (i, 0, 0)),
        out_shape=jax.ShapeDtypeStruct((per, total, width), jnp.bfloat16),
        cost_estimate=block_cost(2 * per * total, total, width, hidden),
        name="inter",
    )(spread, *inter)
    summed = summed.reshape(per, seq_count, stretches, width)
    final = pl.pallas_call(
        functools.partial(return_kernel, seq_count, mp_count),
        in_specs=[any_space],
        out_specs=any_space,
        out_shape=jax.ShapeDtypeStruct((seq_count, mp_count, per, stretches, width), jnp.bfloat16),
        scratch_shapes=[
            pltpu.SemaphoreType.DMA((seq_count - 1,)),
            pltpu.SemaphoreType.DMA((seq_count - 1,)),
            pltpu.SemaphoreType.DMA((seq_count, mp_count - 1)),
            pltpu.SemaphoreType.DMA((seq_count, mp_count - 1)),
            pltpu.SemaphoreType.DMA,
        ],
        compiler_params=pltpu.CompilerParams(collective_id=1, has_side_effects=True),
        name="hand_back",
    )(summed)
    final = jnp.transpose(final.reshape(count * per, stretches, width)[:hop], (1, 0, 2))
    return final.reshape(stretches * hop, width)


def solution(mesh):
    return jax.shard_map(
        on_device,
        mesh=mesh,
        in_specs=(
            P("seq", None, None),
            P(None, None, "mp"),
            P("mp", None),
            P(None, "mp"),
            P("mp", None),
            P(None, None, "mp"),
            P("mp", None),
            P(None, "mp"),
            P("mp", None),
        ),
        out_specs=P("seq", None),
        check_vma=False,
    )
```

```python
import functools

import jax
import jax.numpy as jnp
from jax import lax
from jax.experimental import pallas as pl
from jax.experimental.pallas import tpu as pltpu
from jax.sharding import PartitionSpec as P

HEADS = 8
HD = 32
LANES = 128
TILE = 8
MESH = pl.DeviceIdType.MESH


def normed_rows(values):
    centre = values - jnp.mean(values, axis=-1, keepdims=True)
    spread = jnp.mean(centre * centre, axis=-1, keepdims=True)
    return (centre * lax.rsqrt(spread + 1e-05)).astype(jnp.bfloat16)


def dot(a, b):
    return jnp.dot(a, b, preferred_element_type=jnp.float32)


def dot_t(a, b):
    return lax.dot_general(a, b, (((1,), (1,)), ((), ())), preferred_element_type=jnp.float32)


def block_rows(rows, packed, heads_width, bias):
    width = rows.shape[-1]
    peers = packed.shape[0]
    up_at = 4 * heads_width
    down_at = up_at + width

    def joined(part):
        at = part * heads_width
        return jnp.concatenate([packed[i, at : at + heads_width] for i in range(peers)], axis=0)

    wide = rows.astype(jnp.float32)
    normed = normed_rows(wide)
    query, key, value = (dot_t(normed, joined(t)).astype(jnp.bfloat16) for t in range(3))
    lane_head = lax.broadcasted_iota(jnp.int32, (1, LANES), 1) // HD
    groups = []
    for g in range(width // LANES):
        q, k, v = (member[:, g * LANES : (g + 1) * LANES] for member in (query, key, value))
        total = None
        for h in range(LANES // HD):
            own = (lane_head == h).astype(jnp.float32)
            scores = dot_t(q * own.astype(jnp.bfloat16), k)
            if bias is not None:
                scores = scores + bias
            scores = scores - jnp.max(scores, axis=-1, keepdims=True)
            weights = jnp.exp(scores * (HD**-0.5))
            scale = 1.0 / jnp.sum(weights, axis=-1, keepdims=True)
            part = dot(weights.astype(jnp.bfloat16), v) * (scale * own)
            total = part if total is None else total + part
        groups.append(total.astype(jnp.bfloat16))
    attended = jnp.concatenate(groups, axis=-1)
    middle = (wide + dot(attended, joined(3))).astype(jnp.bfloat16)
    wide = middle.astype(jnp.float32)
    normed = normed_rows(wide)
    branch = None
    for i in range(peers):
        hidden = jnp.maximum(dot(normed, packed[i, up_at:down_at]), 0.0).astype(jnp.bfloat16)
        part = dot(hidden, packed[i, down_at:])
        branch = part if branch is None else branch + part
    return wide + branch


def source_of(slots, hop, per):
    r = slots // (2 * per) * per + slots % per
    return jnp.where(r < hop, r + jnp.where(slots % (2 * per) < per, 0, hop), -1)


def intra_kernel(hop, per, heads_width, x_ref, packed, o_ref):
    frames = x_ref.shape[1]
    peers = o_ref.shape[0]
    padded = peers * 2 * per
    source = source_of(lax.broadcasted_iota(jnp.int32, (padded, frames), 0), hop, per)
    pick = (source == lax.broadcasted_iota(jnp.int32, (padded, frames), 1)).astype(jnp.bfloat16)
    rows = dot(pick, x_ref[0]).astype(jnp.bfloat16)
    keys = source_of(lax.broadcasted_iota(jnp.int32, (1, padded), 1), hop, per)
    bias = jnp.where(keys >= 0, 0.0, -1e30).astype(jnp.float32)
    result = block_rows(rows, packed, heads_width, bias)
    o_ref[:, 0] = result.reshape(peers, 2 * per, result.shape[-1]).astype(o_ref.dtype)


def inter_kernel(heads_width, x_ref, packed, o_ref):
    ends = []
    for half in range(2):
        result = block_rows(x_ref[half, 0], packed, heads_width, None)
        ends.append(result.astype(jnp.bfloat16).astype(jnp.float32))
    first, second = ends
    moved = pltpu.roll(second, 1, 0)
    moved = jnp.where(lax.broadcasted_iota(jnp.int32, moved.shape, 0) == 0, 0.0, moved)
    o_ref[0] = (first + moved).astype(o_ref.dtype)


def greet(ids):
    barrier = pltpu.get_barrier_semaphore()
    for peer in ids:
        pl.semaphore_signal(barrier, inc=1, device_id=peer, device_id_type=MESH)
    pl.semaphore_wait(barrier, len(ids))


def exchange_kernel(seq_count, mp_count, src, dst, send, recv, local):
    count = seq_count * mp_count
    me = lax.axis_index("seq") * mp_count + lax.axis_index("mp")
    ranks = [lax.rem(me + k, count) for k in range(1, count)]
    greet([(rank // mp_count, lax.rem(rank, mp_count)) for rank in ranks])
    own = pltpu.make_async_copy(src.at[me], dst.at[me], local)
    own.start()
    copies = []
    for k, rank in enumerate(ranks):
        copies.append(
            pltpu.make_async_remote_copy(
                src_ref=src.at[rank],
                dst_ref=dst.at[me],
                send_sem=send.at[k],
                recv_sem=recv.at[k],
                device_id=(rank // mp_count, lax.rem(rank, mp_count)),
                device_id_type=MESH,
            )
        )
        copies[-1].start()
    own.wait()
    for copy in copies:
        copy.wait()


def line_step(mp_count, by, upward):
    mp = lax.axis_index("mp")
    if upward:
        return (mp >= by) & (mp + 1 < mp_count), (mp - by + mp_count) % mp_count, (mp + 1) % mp_count
    return (mp + by < mp_count) & (mp >= 1), (mp + by) % mp_count, (mp - 1 + mp_count) % mp_count


def line_arrival(mp_count, by, upward):
    mp = lax.axis_index("mp")
    if upward:
        return mp >= by, (mp - by + mp_count) % mp_count
    return mp + by < mp_count, (mp + by) % mp_count


def gather_kernel(seq_count, mp_count, intra, inter, intra_all, inter_all, send, recv, side_send, side_recv, local):
    seq, mp = lax.axis_index("seq"), lax.axis_index("mp")
    half = seq % 2
    partner = seq + 1 - 2 * half
    greet([(seq, (mp + k) % mp_count) for k in range(1, mp_count)] + [(partner, mp)])
    sources, gathers = (intra, inter), (intra_all, inter_all)
    own = [pltpu.make_async_copy(sources[w], gathers[w].at[mp], local.at[w]) for w in range(2)]
    for copy in own:
        copy.start()

    def along(by, upward, w):
        go, slot, peer = line_step(mp_count, by, upward)
        side = int(upward)
        return go, pltpu.make_async_remote_copy(
            src_ref=sources[w].at[half] if by == 0 else gathers[w].at[slot, half],
            dst_ref=gathers[w].at[slot, half],
            send_sem=send.at[side, by, w],
            recv_sem=recv.at[side, by, w],
            device_id=(seq, peer),
            device_id_type=MESH,
        )

    def across(by, upward, w):
        there, slot = line_arrival(mp_count, by, upward)
        side = int(upward)
        return there, pltpu.make_async_remote_copy(
            src_ref=gathers[w].at[slot, half],
            dst_ref=gathers[w].at[slot, half],
            send_sem=side_send.at[side, by - 1, w],
            recv_sem=side_recv.at[side, by - 1, w],
            device_id=(partner, mp),
            device_id_type=MESH,
        )

    for by in range(mp_count):
        for w in range(2):
            for upward in (False, True):
                if by > 0:
                    there, copy = across(by, upward, w)
                    _, arrived = along(by - 1, upward, w)

                    @pl.when(there)
                    def _():
                        arrived.wait_recv()
                        copy.start()

                if by < mp_count - 1:
                    go, onward = along(by, upward, w)

                    @pl.when(go)
                    def _():
                        onward.start()

    for copy in own:
        copy.wait()
    for by in range(mp_count):
        for w in range(2):
            for upward in (False, True):
                if by > 0:
                    there, copy = across(by, upward, w)

                    @pl.when(there)
                    def _():
                        copy.wait()

                if by < mp_count - 1:
                    go, onward = along(by, upward, w)

                    @pl.when(go)
                    def _():
                        onward.wait_send()


def return_kernel(seq_count, mp_count, src, dst, send, recv, send_on, recv_on, local):
    seq, mp = lax.axis_index("seq"), lax.axis_index("mp")
    across = [lax.rem(seq + k, seq_count) for k in range(1, seq_count)]
    greet([(peer, mp) for peer in across] + [(seq, (mp + k) % mp_count) for k in range(1, mp_count)])
    own = pltpu.make_async_copy(src.at[:, seq], dst.at[seq, mp], local)
    own.start()
    copies = []
    for k, peer in enumerate(across):
        copies.append(
            pltpu.make_async_remote_copy(
                src_ref=src.at[:, peer],
                dst_ref=dst.at[seq, mp],
                send_sem=send.at[k],
                recv_sem=recv.at[k],
                device_id=(peer, mp),
                device_id_type=MESH,
            )
        )
        copies[-1].start()

    def along(by, upward, k):
        go, slot, peer = line_step(mp_count, by, upward)
        slab = dst.at[(seq + seq_count - k) % seq_count, slot]
        return go, pltpu.make_async_remote_copy(
            src_ref=slab,
            dst_ref=slab,
            send_sem=send_on.at[int(upward), by, k],
            recv_sem=recv_on.at[int(upward), by, k],
            device_id=(seq, peer),
            device_id_type=MESH,
        )

    for by in range(mp_count):
        for k in range(seq_count):
            if by == 0:
                if k == 0:
                    own.wait()
                else:
                    copies[k - 1].wait_recv()
            for upward in (False, True):
                if by > 0:
                    _, arrived = along(by - 1, upward, k)

                    @pl.when(line_arrival(mp_count, by, upward)[0])
                    def _():
                        arrived.wait_recv()

                if by < mp_count - 1:
                    go, onward = along(by, upward, k)

                    @pl.when(go)
                    def _():
                        onward.start()

    for copy in copies:
        copy.wait_send()
    for by in range(mp_count - 1):
        for k in range(seq_count):
            for upward in (False, True):
                go, onward = along(by, upward, k)

                @pl.when(go)
                def _():
                    onward.wait_send()


def packed_shard(qkv, out, up, down):
    width = qkv.shape[0]
    turned = jnp.transpose(qkv, (1, 2, 0)).reshape(-1, width)
    return jnp.concatenate([turned, out, up, down], axis=0).reshape(2, -1, width)


def whole(array):
    return pl.BlockSpec(array.shape, lambda i: (0,) * array.ndim)


def block_cost(rows, per_group, width, hidden):
    flops = 2 * rows * (width * width * 4 + width * hidden * 2 + 8 * LANES * per_group)
    return pl.CostEstimate(flops=flops, bytes_accessed=rows * width * 4, transcendentals=rows * per_group * 8)


def on_device(
    frames, intra_qkv, intra_out, intra_up, intra_down, inter_qkv, inter_out, inter_up, inter_down
):
    seq_count = lax.axis_size("seq")
    mp_count = lax.axis_size("mp")
    count = seq_count * mp_count
    stretches, length, width = frames.shape
    hop = length // 2
    per = -(-hop // count)
    per = -(-per // (TILE // 2)) * (TILE // 2)
    share = stretches // mp_count
    heads_width = intra_qkv.shape[2]
    hidden = intra_up.shape[1] * mp_count
    any_space = pl.BlockSpec(memory_space=pl.ANY)
    shards = (
        packed_shard(intra_qkv, intra_out, intra_up, intra_down),
        packed_shard(inter_qkv, inter_out, inter_up, inter_down),
    )
    semaphores = pltpu.SemaphoreType.DMA((2, mp_count - 1, 2))
    intra, inter = pl.pallas_call(
        functools.partial(gather_kernel, seq_count, mp_count),
        in_specs=[any_space] * 2,
        out_specs=[any_space] * 2,
        out_shape=[jax.ShapeDtypeStruct((mp_count,) + shards[0].shape, jnp.bfloat16)] * 2,
        scratch_shapes=[semaphores] * 4 + [pltpu.SemaphoreType.DMA((2,))],
        compiler_params=pltpu.CompilerParams(collective_id=2, has_side_effects=True),
        name="gather",
    )(*shards)
    intra = intra.reshape(mp_count, -1, width)
    inter = inter.reshape(mp_count, -1, width)
    own = lax.dynamic_slice_in_dim(frames, lax.axis_index("mp") * share, share, 0)
    parted = pl.pallas_call(
        functools.partial(intra_kernel, hop, per, heads_width),
        grid=(share,),
        in_specs=[pl.BlockSpec((1, length, width), lambda i: (i, 0, 0))] + [whole(intra)],
        out_specs=pl.BlockSpec((count, 1, 2 * per, width), lambda i: (0, i, 0, 0)),
        out_shape=jax.ShapeDtypeStruct((count, share, 2 * per, width), jnp.bfloat16),
        cost_estimate=block_cost(share * length, length, width, hidden),
        name="intra",
    )(own, intra)
    spread = pl.pallas_call(
        functools.partial(exchange_kernel, seq_count, mp_count),
        in_specs=[any_space],
        out_specs=any_space,
        out_shape=jax.ShapeDtypeStruct(parted.shape, jnp.bfloat16),
        scratch_shapes=[
            pltpu.SemaphoreType.DMA((count - 1,)),
            pltpu.SemaphoreType.DMA((count - 1,)),
            pltpu.SemaphoreType.DMA,
        ],
        compiler_params=pltpu.CompilerParams(collective_id=0, has_side_effects=True),
        name="exchange",
    )(parted)
    total = count * share
    spread = jnp.transpose(spread.reshape(total, 2, per, width), (1, 2, 0, 3))
    summed = pl.pallas_call(
        functools.partial(inter_kernel, heads_width),
        grid=(per,),
        in_specs=[pl.BlockSpec((2, 1, total, width), lambda i: (0, i, 0, 0))]
        + [whole(inter)],
        out_specs=pl.BlockSpec((1, total, width), lambda i: (i, 0, 0)),
        out_shape=jax.ShapeDtypeStruct((per, total, width), jnp.bfloat16),
        cost_estimate=block_cost(2 * per * total, total, width, hidden),
        name="inter",
    )(spread, inter)
    summed = summed.reshape(per, seq_count, stretches, width)
    final = pl.pallas_call(
        functools.partial(return_kernel, seq_count, mp_count),
        in_specs=[any_space],
        out_specs=any_space,
        out_shape=jax.ShapeDtypeStruct((seq_count, mp_count, per, stretches, width), jnp.bfloat16),
        scratch_shapes=[
            pltpu.SemaphoreType.DMA((seq_count - 1,)),
            pltpu.SemaphoreType.DMA((seq_count - 1,)),
            pltpu.SemaphoreType.DMA((2, mp_count - 1, seq_count)),
            pltpu.SemaphoreType.DMA((2, mp_count - 1, seq_count)),
            pltpu.SemaphoreType.DMA,
        ],
        compiler_params=pltpu.CompilerParams(collective_id=1, has_side_effects=True),
        name="hand_back",
    )(summed)
    final = jnp.transpose(final.reshape(count * per, stretches, width)[:hop], (1, 0, 2))
    return final.reshape(stretches * hop, width)


def solution(mesh):
    return jax.shard_map(
        on_device,
        mesh=mesh,
        in_specs=(
            P("seq", None, None),
            P(None, None, "mp"),
            P("mp", None),
            P(None, "mp"),
            P("mp", None),
            P(None, None, "mp"),
            P("mp", None),
            P(None, "mp"),
            P("mp", None),
        ),
        out_specs=P("seq", None),
        check_vma=False,
    )
```
